64 devices in a mesh: rep: 4 (over x, y), seq: 16 (over z, core).
Axes of the slice: x: 2, y: 2, z: 8, core: 2. Of those that a mesh axis runs over, the one named last changes fastest.
The devices are a block of a 4x4x8 slice.
Arguments:
- hidden: bfloat16 [128, 5120], P('rep'), parts along dimension 0
- w_query: bfloat16 [5120, 4096], replicated
- w_key: bfloat16 [5120, 1024], replicated
- w_value: bfloat16 [5120, 1024], replicated
- w_out: bfloat16 [4096, 5120], P('seq')
- k_cache: bfloat16 [128, 1024, 8, 128], P('rep', 'seq'), parts along dimension 0
- v_cache: bfloat16 [128, 1024, 8, 128], P('rep', 'seq'), parts along dimension 0
- positions: int32 [128], P('rep'), parts along dimension 0
Outputs:
- output 1: bfloat16 [128, 5120], P('rep'), parts along dimension 0
- output 2: bfloat16 [128, 1024, 8, 128], P('rep', 'seq'), parts along dimension 0
- output 3: bfloat16 [128, 1024, 8, 128], P('rep', 'seq'), parts along dimension 0
There are 4 independent parts. The reference program is written for one: setup_inputs(seed, part) draws one part's arguments, and reference() takes and returns one part's arrays. A program takes and returns all parts, laid end to end along the dimension named above; an argument that names none is the same for every part.
All inputs are finite; a program needn't handle non-finite values.
Results may differ from the reference program's by a relative error of at most 0.00606072.
Values are sent between devices in bfloat16 or wider.
A program may use at most 768 MiB of HBM per device.

```python
import math
import jax
import jax.numpy as jnp
from jax import lax

D_MODEL = 5120
NUM_HEADS = 32
KV_HEADS = 8
HEAD_DIM = 128
BATCH_SIZE = 32
LOCAL_LEN = 64
SEQ_LEN = 1024


def query_shift(hidden, w_query):
    group_size = NUM_HEADS // KV_HEADS
    q_flat = jnp.dot(hidden, w_query, preferred_element_type=jnp.float32).astype(jnp.bfloat16).astype(jnp.float32)
    q_heads = q_flat.reshape(BATCH_SIZE, KV_HEADS, group_size, HEAD_DIM)
    gram_mat = jnp.einsum('bkgd,bkhd->bkgh', q_heads, q_heads)
    coeffs = jnp.linalg.solve(gram_mat, jnp.ones((BATCH_SIZE, KV_HEADS, group_size, 1), jnp.float32))
    score_drop = math.log(SEQ_LEN) - 1.0
    return -score_drop * HEAD_DIM ** 0.5 * jnp.einsum('bkgo,bkgd->bkd', coeffs, q_heads)


def setup_inputs(seed: int = 0, part: int = 0) -> dict:
    root = jax.random.key(seed)
    shared = jax.random.split(root, 4)
    part_keys = jax.random.split(jax.random.fold_in(root, part), 6)
    blocks = SEQ_LEN // LOCAL_LEN
    block_shape = (BATCH_SIZE, blocks, LOCAL_LEN, KV_HEADS, HEAD_DIM)
    cache_shape = (BATCH_SIZE, SEQ_LEN, KV_HEADS, HEAD_DIM)
    q_width = NUM_HEADS * HEAD_DIM
    kv_width = KV_HEADS * HEAD_DIM
    hidden = jax.random.normal(part_keys[0], (BATCH_SIZE, D_MODEL), jnp.float32).astype(jnp.bfloat16)
    w_query = (jax.random.normal(shared[0], (D_MODEL, q_width), jnp.float32) * D_MODEL ** -0.5).astype(jnp.bfloat16)
    w_key = (jax.random.normal(shared[1], (D_MODEL, kv_width), jnp.float32) * D_MODEL ** -0.5).astype(jnp.bfloat16)
    w_value = (jax.random.normal(shared[2], (D_MODEL, kv_width), jnp.float32) * D_MODEL ** -0.5).astype(jnp.bfloat16)
    w_out = (jax.random.normal(shared[3], (q_width, D_MODEL), jnp.float32) * q_width ** -0.5).astype(jnp.bfloat16)
    key_scale = jax.random.uniform(part_keys[1], (BATCH_SIZE, blocks, 1, KV_HEADS, 1), jnp.float32, 0.5, 1.5)
    key_noise = jax.random.normal(part_keys[2], block_shape, jnp.float32) * key_scale
    k_cache = key_noise.reshape(cache_shape) + query_shift(hidden, w_query)[:, None]
    v_base = jax.random.normal(part_keys[3], (BATCH_SIZE, blocks, 1, KV_HEADS, HEAD_DIM), jnp.float32)
    v_cache = (v_base + jax.random.normal(part_keys[4], block_shape, jnp.float32)).reshape(cache_shape)
    positions = jax.random.randint(part_keys[5], (BATCH_SIZE,), SEQ_LEN // 4, SEQ_LEN, dtype=jnp.int32)
    return {'hidden': hidden, 'w_query': w_query, 'w_key': w_key, 'w_value': w_value, 'w_out': w_out, 'k_cache': k_cache.astype(jnp.bfloat16), 'v_cache': v_cache.astype(jnp.bfloat16), 'positions': positions}


def reference(hidden, w_query, w_key, w_value, w_out, k_cache, v_cache, positions):
    group_size = NUM_HEADS // KV_HEADS
    q_flat = jnp.dot(hidden, w_query, preferred_element_type=jnp.float32).astype(jnp.bfloat16)
    key_new = jnp.dot(hidden, w_key, preferred_element_type=jnp.float32).astype(jnp.bfloat16).reshape(BATCH_SIZE, KV_HEADS, HEAD_DIM)
    value_new = jnp.dot(hidden, w_value, preferred_element_type=jnp.float32).astype(jnp.bfloat16).reshape(BATCH_SIZE, KV_HEADS, HEAD_DIM)
    seq_ids = jnp.arange(SEQ_LEN)
    at_pos = (seq_ids[None, :] == positions[:, None])[:, :, None, None]
    k_updated = jnp.where(at_pos, key_new[:, None], k_cache)
    v_updated = jnp.where(at_pos, value_new[:, None], v_cache)
    is_valid = seq_ids[None, :] <= positions[:, None]
    q_heads = q_flat.astype(jnp.float32).reshape(BATCH_SIZE, KV_HEADS, group_size, HEAD_DIM)

    def one_row(row_args):
        q_row, k_row, v_row, valid_row = row_args
        scores = jnp.einsum('kgd,skd->kgs', q_row, k_row.astype(jnp.float32)) * HEAD_DIM ** -0.5
        scores = jnp.where(valid_row[None, None, :], scores, -jnp.inf)
        weights = jax.nn.softmax(scores, axis=-1)
        return jnp.einsum('kgs,skd->kgd', weights, v_row.astype(jnp.float32))

    attended = lax.map(one_row, (q_heads, k_updated, v_updated, is_valid))
    combined = attended.reshape(BATCH_SIZE, NUM_HEADS * HEAD_DIM).astype(jnp.bfloat16)
    result = jnp.dot(combined, w_out, preferred_element_type=jnp.float32).astype(jnp.bfloat16)
    return result, k_updated, v_updated
```

```python
import functools

import jax
import jax.numpy as jnp
from jax import lax
from jax.experimental import pallas as pl
from jax.experimental.pallas import tpu as pltpu
from jax.sharding import PartitionSpec as P

MESH = pl.DeviceIdType.MESH
BF16 = jnp.bfloat16
F32 = jnp.float32
NEG = float('-inf')
DMA = pltpu.SemaphoreType.DMA
NT = (((1,), (1,)), ((), ()))


def place(n_chips):
    me = lax.axis_index('seq')
    chip = lax.div(me, 2)
    core = lax.rem(me, 2)
    return chip, core, me + 1 - 2 * core


def remote(src, dst, send, recv, dev):
    return pltpu.make_async_remote_copy(src_ref=src, dst_ref=dst, send_sem=send, recv_sem=recv,
                                        device_id={'seq': dev}, device_id_type=MESH)


def greet(peers):
    barrier = pltpu.get_barrier_semaphore()
    for p in peers:
        pl.semaphore_signal(barrier, inc=1, device_id={'seq': p}, device_id_type=MESH)
    return lambda: pl.semaphore_wait(barrier, len(peers))


def project_kernel(n_chips, pieces, width, x_hbm, wq, wk, wv, k_hbm, v_hbm, g_ref, k_out, v_out,
                   x_ref, wbuf, xsem, wsem, csem, send_sem, recv_sem):
    chip, core, sibling = place(n_chips)
    parity = lax.rem(chip, 2)
    shard = 2 * parity + core
    right = lax.rem(chip + 1, n_chips)
    left = lax.rem(chip + n_chips - 1, n_chips)
    arrived = greet([sibling, 2 * right, 2 * right + 1, 2 * left, 2 * left + 1])
    nq = pieces - 2

    def load(p):
        src, col = (wq, (shard * nq + p) * width) if p < nq else ((wk, wv)[p - nq], shard * width)
        return pltpu.make_async_copy(src.at[:, pl.ds(pl.multiple_of(col, 128), width)], wbuf.at[p], wsem.at[p])

    load_x = pltpu.make_async_copy(x_hbm, x_ref, xsem)
    load_x.start()
    ahead = 3
    for p in range(ahead):
        load(p).start()
    caches = [pltpu.make_async_copy(k_hbm, k_out, csem.at[0]), pltpu.make_async_copy(v_hbm, v_out, csem.at[1])]
    load_x.wait()
    x = x_ref[...]
    sends = []
    for p in range(pieces):
        load(p).wait()
        if p + ahead < pieces:
            load(p + ahead).start()
        elif p + ahead - pieces < 2:
            caches[p + ahead - pieces].start()
        acc = jnp.dot(x, wbuf[p], preferred_element_type=F32)
        g_ref[shard, p] = acc.astype(BF16)
        if p == 0:
            arrived()
        block = g_ref.at[shard, p]
        near = right if p % 2 == 0 else left
        for s, (dev, slot) in enumerate([(sibling, 0), (2 * near, 1 + core), (2 * near + 1, 1 + core)]):
            copy = remote(block, block, send_sem.at[p, s], recv_sem.at[p, slot], dev)
            copy.start()
            sends.append(copy)
    for p in range(pieces):
        for s in range(3):
            owner = 2 * parity + 1 - core if s == 0 else 2 * (1 - parity) + s - 1
            block = g_ref.at[owner, p]
            remote(block, block, send_sem.at[p, s], recv_sem.at[p, s], sibling).wait_recv()
    for copy in sends:
        copy.wait_send()
    for copy in caches:
        copy.wait()


def patch_kernel(length, kv_heads, pos_ref, g_ref, k_in, v_in, k_ref, v_ref, rows):
    batch = k_ref.shape[0]
    dim = k_ref.shape[-1]
    shards, pieces = g_ref.shape[:2]
    per = kv_heads // shards
    base = lax.axis_index('seq') * length
    for kind in range(2):
        for h in range(kv_heads):
            part = g_ref[h // per, pieces - 2 + kind]
            lo = (h % per) * dim
            rows[kind, pl.ds(h, batch, stride=kv_heads), :] = part[:, lo:lo + dim].astype(F32)
    for b in range(batch):
        p = pos_ref[b] - base

        @pl.when((p >= 0) & (p < length))
        def _():
            for kind, ref in ((0, k_ref), (1, v_ref)):
                ref[b, p] = rows[kind, kv_heads * b:kv_heads * (b + 1), :].astype(BF16)


MSG = 72


def attend_kernel(n_chips, kv_heads, scale, length, pos_ref, g_ref, k_ref, v_ref, wo_hbm, y_ref,
                  qs, tmat, obuf, sbuf, mbuf, rbuf, wo, ybuf, ysib, yc, yr, yg, wsem,
                  sa_s, sa_r, sb_s, sb_r, ya_s, ya_r, yb_s, yb_r, ag_s, ag_r, fw_s, fw_r):
    chip, core, sibling = place(n_chips)
    batch, span, dim = k_ref.shape
    heads = 4 * n_chips
    order = sorted(range(1, n_chips), key=lambda d: -min(d, n_chips - d))
    peer = {d: lax.rem(chip + d, n_chips) for d in range(1, n_chips)}
    source = {d: lax.rem(chip + n_chips - d, n_chips) for d in range(1, n_chips)}
    arrived = greet([sibling] + [2 * peer[d] + core for d in order])
    load_wo = pltpu.make_async_copy(wo_hbm, wo, wsem)
    load_wo.start()
    base = lax.axis_index('seq') * length

    half = heads // 2
    per = heads // g_ref.shape[0]
    wide = g_ref.shape[-1]
    for h in range(heads):
        col = (h % per) * dim
        part = g_ref[h // per, col // wide]
        r = (h % 2) * half + h // 2
        qs[pl.ds(r, batch, stride=heads), :] = part[:, col % wide:col % wide + dim].astype(F32)
    row = lax.broadcasted_iota(jnp.int32, (heads, span), 0)
    col = lax.broadcasted_iota(jnp.int32, (heads, span), 1)
    same = lax.div(lax.rem(row, half), heads // kv_heads // 2) == lax.rem(col, kv_heads)
    tmat[...] = jnp.where(same, lax.div(col, kv_heads), 1 << 20)
    lane = lax.broadcasted_iota(jnp.int32, (heads, dim), 1)

    unroll = 4

    def group(i, carry):
        mst, lst = carry
        for u in range(unroll):
            b = i * unroll + u
            q = qs[pl.ds(pl.multiple_of(b * heads, 8), heads), :].astype(BF16)
            s = lax.dot_general(q, k_ref[b], NT, preferred_element_type=F32) * scale
            s = jnp.where(tmat[...] <= pos_ref[b] - base, s, NEG)
            m = jnp.max(s, axis=1, keepdims=True)
            p = jnp.exp(s - jnp.where(m == NEG, 0.0, m))
            l = jnp.sum(p, axis=1, keepdims=True)
            o = jnp.dot(p.astype(BF16), v_ref[b], preferred_element_type=F32)
            mst = jnp.where(lane == b, m, mst)
            lst = jnp.where(lane == b, l, lst)
            obuf[pl.ds(b, half, stride=MSG), :] = o[:half]
            obuf[pl.ds(b + batch, half, stride=MSG), :] = o[half:]
        return mst, lst

    zero = jnp.zeros((heads, dim), F32)
    mst, lst = lax.fori_loop(0, batch // unroll, group, (zero, zero))
    stat = 2 * batch
    for r, v in enumerate((mst[:half], mst[half:], lst[:half], lst[half:])):
        obuf[pl.ds(stat + r, half, stride=MSG), :] = v
    for r in range(4, 8):
        obuf[pl.ds(stat + r, half, stride=MSG), :] = jnp.zeros((half, dim), F32)
    arrived()

    def message(j):
        return obuf.at[pl.ds(pl.multiple_of(j * MSG, 8), MSG)]

    pair = []
    for t in range(n_chips):
        copy = remote(message(2 * t + 1 - core), sbuf.at[t], sa_s.at[t], sa_r.at[t], sibling)
        copy.start()
        pair.append(copy)
    sub = lax.broadcasted_iota(jnp.int32, (8, dim), 0)
    scales = []
    for t in range(n_chips):
        pair[t].wait_recv()
        mine = obuf[pl.ds(pl.multiple_of((2 * t + core) * MSG + stat, 8), 8), :]
        theirs = sbuf[t, stat:, :]
        top = jnp.maximum(mine, theirs)
        safe = jnp.where(top == NEG, 0.0, top)
        a0, a1 = jnp.exp(mine - safe), jnp.exp(theirs - safe)
        total = pltpu.roll(a0, 2, 0) * mine + pltpu.roll(a1, 2, 0) * theirs
        mbuf[t, stat:, :] = jnp.where(sub < 2, top, jnp.where(sub < 4, total, 0.0))
        scales += [a0, a1]
    cols = jnp.concatenate(scales, axis=0).T
    for t in range(n_chips):
        for hh in range(2):
            lo = hh * batch
            own = obuf[pl.ds(pl.multiple_of((2 * t + core) * MSG + lo, 8), batch), :]
            c = 16 * t + hh
            mbuf[t, lo:lo + batch, :] = (own * cols[:batch, c:c + 1]
                                         + sbuf[t, lo:lo + batch, :] * cols[:batch, c + 8:c + 9])

    sends = []
    for d in order:
        copy = remote(mbuf.at[peer[d]], rbuf.at[chip], sb_s.at[d], sb_r.at[d], 2 * peer[d] + core)
        copy.start()
        sends.append(copy)
    rbuf[chip] = mbuf[chip]
    for d in order:
        remote(mbuf.at[source[d]], rbuf.at[source[d]], sb_s.at[d], sb_r.at[d], 2 * source[d] + core).wait_recv()
    stats = [rbuf[t, stat:, :] for t in range(n_chips)]
    top = functools.reduce(jnp.maximum, stats)
    fac = [jnp.exp(v - top) for v in stats]
    total = functools.reduce(jnp.add, [a * pltpu.roll(v, 6, 0) for a, v in zip(fac, stats)])
    cols = jnp.concatenate([a / total for a in fac] + [jnp.zeros((128 - 8 * n_chips, dim), F32)], axis=0).T
    outs = []
    for hh in range(2):
        lo = hh * batch
        outs.append(functools.reduce(jnp.add, [
            rbuf[t, lo:lo + batch, :] * cols[:batch, 8 * t + hh:8 * t + hh + 1] for t in range(n_chips)]))
    combined = jnp.concatenate(outs, axis=1).astype(BF16)
    for copy in pair + sends:
        copy.wait_send()

    load_wo.wait()
    quarter = ybuf.shape[-1]
    rows = ybuf.shape[2]

    def product(q):
        cut = wo[:, pl.ds(pl.multiple_of(q * quarter, 128), quarter)]
        out = jnp.dot(combined, cut, preferred_element_type=F32)
        return out.reshape(batch // rows, rows, quarter)

    pair = []
    for e in range(2):
        q = 2 * (1 - core) + e
        ybuf[q] = product(q)
        copy = remote(ybuf.at[q], ysib.at[e], ya_s.at[e], ya_r.at[e], sibling)
        copy.start()
        pair.append(copy)
    groups = batch // rows
    for e in range(2):
        q = 2 * core + e
        ybuf[q] = product(q)
    for e in range(2):
        pair[e].wait_recv()
        yc[groups * e:groups * (e + 1)] = ybuf[2 * core + e] + ysib[e]
    sends = []
    for d in order:
        copy = remote(yc.at[peer[d]], yr.at[chip], yb_s.at[d], yb_r.at[d], 2 * peer[d] + core)
        copy.start()
        sends.append(copy)
    acc = yc[chip]
    for d in order:
        remote(yc.at[source[d]], yr.at[source[d]], yb_s.at[d], yb_r.at[d], 2 * source[d] + core).wait_recv()
        acc = acc + yr[source[d]]
    yg[core, chip] = acc.astype(BF16)
    for copy in pair + sends:
        copy.wait_send()

    sends = []
    piece = yg.at[core, chip]
    for d in order:
        copy = remote(piece, piece, ag_s.at[d], ag_r.at[d], 2 * peer[d] + core)
        copy.start()
        sends.append(copy)
    copy = remote(piece, piece, fw_s.at[0], fw_r.at[0], sibling)
    copy.start()
    sends.append(copy)
    for d in order:
        got = yg.at[core, source[d]]
        remote(got, got, ag_s.at[d], ag_r.at[d], 2 * source[d] + core).wait_recv()
        copy = remote(got, got, fw_s.at[d], fw_r.at[d], sibling)
        copy.start()
        sends.append(copy)
    for d in [0] + order:
        got = yg.at[1 - core, chip if d == 0 else source[d]]
        remote(got, got, fw_s.at[d], fw_r.at[d], sibling).wait_recv()
    for k in range(2):
        for t in range(n_chips):
            q = 2 * k + t // groups
            lo = rows * (t % groups)
            y_ref[lo:lo + rows, q * quarter:(q + 1) * quarter] = yg[k, t]
    for copy in sends:
        copy.wait_send()


def solution(mesh):
    cache_spec = P('rep', 'seq', None, None)
    in_specs = (P('rep', None), P(), P(), P(), P('seq', None), cache_spec, cache_spec, P('rep'))
    out_specs = (P('rep', None), cache_spec, cache_spec)
    n_seq = mesh.shape['seq']
    n_chips = n_seq // 2

    def local_step(hidden, w_query, w_key, w_value, w_out, k_cache, v_cache, positions):
        batch, length, kv_heads, dim = k_cache.shape
        model, q_width = w_query.shape
        heads = q_width // dim
        width = kv_heads * dim // 4
        nq = q_width // 4 // width
        pieces = nq + 2
        vm = pl.BlockSpec(memory_space=pltpu.VMEM)
        hbm = pl.BlockSpec(memory_space=pltpu.HBM)
        smem = pl.BlockSpec(memory_space=pltpu.SMEM)
        stay = lambda a: pltpu.with_memory_space_constraint(a, pltpu.HBM)
        gathered, k_held, v_held = pl.pallas_call(
            functools.partial(project_kernel, n_chips, pieces, width),
            out_shape=(pltpu.VMEM((4, pieces, batch, width), BF16),
                       pltpu.VMEM(k_cache.shape, BF16), pltpu.VMEM(v_cache.shape, BF16)),
            in_specs=[hbm] * 6,
            out_specs=(vm, vm, vm),
            scratch_shapes=[pltpu.VMEM(hidden.shape, BF16), pltpu.VMEM((pieces, model, width), BF16),
                            DMA, DMA((pieces,)), DMA((2,)),
                            DMA((pieces, 3)), DMA((pieces, 3))],
            compiler_params=pltpu.CompilerParams(collective_id=0, has_side_effects=True, vmem_limit_bytes=40 << 20),
            name='project',
        )(*map(stay, (hidden, w_query, w_key, w_value, k_cache, v_cache)))

        k_new, v_new = pl.pallas_call(
            functools.partial(patch_kernel, length, kv_heads),
            out_shape=(pltpu.VMEM(k_cache.shape, BF16), pltpu.VMEM(v_cache.shape, BF16)),
            in_specs=[smem, vm, vm, vm],
            out_specs=(vm, vm),
            scratch_shapes=[pltpu.VMEM((2, batch * kv_heads, dim), F32)],
            input_output_aliases={2: 0, 3: 1},
            compiler_params=pltpu.CompilerParams(vmem_limit_bytes=32 << 20),
            name='patch',
        )(positions, gathered, k_held, v_held)

        rows = batch * 4 // n_chips // 2
        quarter = model // 4
        span = length * kv_heads
        f = lambda *shape: pltpu.VMEM(shape, F32)
        result = pl.pallas_call(
            functools.partial(attend_kernel, n_chips, kv_heads, dim ** -0.5, length),
            out_shape=jax.ShapeDtypeStruct((batch, model), BF16),
            in_specs=[smem, vm, vm, vm, hbm],
            out_specs=vm,
            scratch_shapes=[
                f(heads * batch, dim), pltpu.VMEM((heads, span), jnp.int32),
                f(n_seq * MSG, dim), f(n_chips, MSG, dim), f(n_chips, MSG, dim), f(n_chips, MSG, dim),
                pltpu.VMEM(w_out.shape, BF16),
                f(4, batch // rows, rows, quarter), f(2, batch // rows, rows, quarter),
                f(n_chips, rows, quarter), f(n_chips, rows, quarter),
                pltpu.VMEM((2, n_chips, rows, quarter), BF16), DMA,
            ] + [DMA((n_chips,))] * 4 + [DMA((2,))] * 2 + [DMA((n_chips,))] * 6,
            compiler_params=pltpu.CompilerParams(collective_id=1, has_side_effects=True, vmem_limit_bytes=40 << 20),
            name='attend',
        )(positions, gathered, k_new.reshape(batch, span, dim), v_new.reshape(batch, span, dim), stay(w_out))
        return result, k_new, v_new

    return jax.shard_map(local_step, mesh=mesh, in_specs=in_specs, out_specs=out_specs, check_vma=False)
```
